32 devices in a mesh: grp: 2 (over x), seq: 16 (over z, y, core).
Axes of the slice: x: 2, y: 2, z: 4, core: 2. Of those that a mesh axis runs over, the one named last changes fastest.
Arguments:
- queries: bfloat16 [16384, 4096], P(('grp', 'seq')), parts along dimension 0, may hold values from -40 to 40
- kv_cache: bfloat16 [2, 16384, 1024], P(None, ('grp', 'seq')), parts along dimension 1, may hold values from -4 to 4
- question: bfloat16 [64, 4096], P('grp'), parts along dimension 0, may hold values from -40 to 40
Outputs:
- context_out: bfloat16 [16384, 4096], P(('grp', 'seq')), parts along dimension 0
- answer: bfloat16 [64, 4096], P(('grp', 'seq')), parts along dimension 0
The draws below stay inside these ranges and needn't reach their ends.
There are 2 independent parts, one for each index of `grp`. The reference program is written for one: setup_inputs(seed, part) draws one part's arguments, and reference() takes and returns one part's arrays. A program takes and returns all parts, laid end to end along the dimension named above; each array names one. Nothing has to cross between parts.
All inputs are finite; a program needn't handle non-finite values.
Results may differ from the reference program's by a relative error of at most 0.004.
Values may be sent and summed in bfloat16 or wider, within the bound.
A program may use at most 256 MiB of HBM per device.

```python
import jax
import jax.numpy as jnp
from jax import lax

HEADS = 32
KV_HEADS = 8
HEAD = 128
TOK_DEV = 512
TOKENS = 8192
QROWS = 32


def drawn_fields(key):
    q_width = HEADS * HEAD
    k_width = KV_HEADS * HEAD
    streams = [jax.random.fold_in(key, 301 + offset) for offset in range(16)]
    keys_f = jnp.clip(jax.random.normal(streams[0], (TOKENS, k_width), jnp.float32), -4.0, 4.0)
    queries_f = jnp.clip(1.5 * jax.random.normal(streams[2], (TOKENS, q_width), jnp.float32), -6.0, 6.0)
    question_f = jnp.clip(1.5 * jax.random.normal(streams[4], (QROWS, q_width), jnp.float32), -6.0, 6.0)
    values_f = jnp.clip(jax.random.normal(streams[6], (TOKENS, k_width), jnp.float32), -4.0, 4.0)
    return (queries_f, jnp.stack((keys_f, values_f)), question_f)


def draw_queries(key, part):
    return drawn_fields(key)[0].astype(jnp.bfloat16)


def draw_kv_cache(key, part):
    return drawn_fields(key)[1].astype(jnp.bfloat16)


def draw_question(key, part):
    return drawn_fields(key)[2].astype(jnp.bfloat16)


def setup_inputs(seed: int = 0, part: int = 0) -> dict:
    seeds = jax.random.split(jax.random.key(seed), 4)
    part_keys = jax.random.split(jax.random.fold_in(seeds[3], part), 4)
    return {
        "queries": draw_queries(jax.random.fold_in(jax.random.fold_in(seeds[3], part), 71), part),
        "kv_cache": draw_kv_cache(jax.random.fold_in(jax.random.fold_in(seeds[3], part), 71), part),
        "question": draw_question(jax.random.fold_in(jax.random.fold_in(seeds[3], part), 71), part),
    }


big_negative = -1.0e30


def group_split(rows_in, groups):
    row_count = rows_in.shape[0]
    return rows_in.reshape(row_count, groups, rows_in.shape[1] // groups).transpose(1, 0, 2)


def visible(block_number, row_count, anchor_rows):
    row_pos = lax.broadcasted_iota(jnp.int32, (row_count, anchor_rows + row_count), 0)
    column = lax.broadcasted_iota(jnp.int32, (row_count, anchor_rows + row_count), 1)
    return jnp.where(column < anchor_rows, block_number > 0, column - anchor_rows <= row_pos)


def block_attention(rows_q, keys_all, values_all, allowed):
    groups = keys_all.shape[1] // HEAD
    group_ratio = rows_q.shape[1] // keys_all.shape[1]
    score_scale = HEAD ** -0.5

    def one_group(pieces):
        query_part, key_part, value_part = pieces
        query_part = query_part.reshape(query_part.shape[0], group_ratio, HEAD).astype(jnp.float32)
        scores = jnp.einsum("brd,kd->rbk", query_part, key_part.astype(jnp.float32)) * score_scale
        scores = jnp.where(allowed[None], scores, big_negative)
        highest = jnp.max(scores, axis=2, keepdims=True)
        exponent = jnp.exp(scores - highest)
        totals = jnp.sum(exponent, axis=2)
        soft_weights = lax.optimization_barrier(exponent.astype(jnp.bfloat16))
        mixture = jnp.einsum("rbk,kd->brd", soft_weights.astype(jnp.float32), value_part.astype(jnp.float32))
        mixture = mixture / totals.T[:, :, None]
        return mixture.astype(jnp.bfloat16).reshape(mixture.shape[0], group_ratio * HEAD)

    result = lax.map(one_group, (group_split(rows_q, groups), group_split(keys_all, groups), group_split(values_all, groups)))
    return result.transpose(1, 0, 2).reshape(rows_q.shape[0], rows_q.shape[1])


def block_summary(rows_q, key_block, value_block):
    groups = key_block.shape[1] // HEAD
    group_ratio = rows_q.shape[1] // key_block.shape[1]
    score_scale = HEAD ** -0.5
    row_count = rows_q.shape[0]

    def one_group(pieces):
        query_part, key_part, value_part = pieces
        query_part = query_part.reshape(row_count, group_ratio, HEAD).astype(jnp.float32)
        scores = jnp.einsum("qrd,kd->rqk", query_part, key_part.astype(jnp.float32)) * score_scale
        highest = jnp.max(scores, axis=2)
        exponent = jnp.exp(scores - highest[:, :, None])
        totals = jnp.sum(exponent, axis=2)
        soft_weights = lax.optimization_barrier(exponent.astype(jnp.bfloat16))
        mixture = jnp.einsum("rqk,kd->qrd", soft_weights.astype(jnp.float32), value_part.astype(jnp.float32))
        return highest.T, totals.T, mixture

    highs, totals, mixture = lax.map(one_group, (group_split(rows_q, groups), group_split(key_block, groups), group_split(value_block, groups)))
    highs = highs.transpose(1, 0, 2).reshape(row_count, groups * group_ratio)
    totals = totals.transpose(1, 0, 2).reshape(row_count, groups * group_ratio)
    mixture = mixture.transpose(1, 0, 2, 3).reshape(row_count, groups * group_ratio, HEAD)
    return highs, totals, mixture


def reference(queries, kv_cache, question):
    blocks = TOKENS // TOK_DEV
    kv_width = kv_cache.shape[2]
    query_blocks = queries.reshape(blocks, TOK_DEV, queries.shape[1])
    key_blocks = kv_cache[0].reshape(blocks, TOK_DEV, kv_width)
    value_blocks = kv_cache[1].reshape(blocks, TOK_DEV, kv_width)
    anchor_keys = key_blocks[0]
    anchor_values = value_blocks[0]

    def phase_one(pieces):
        block_number, rows_q, own_keys, own_values = pieces
        keys_all = jnp.concatenate((anchor_keys, own_keys), axis=0)
        values_all = jnp.concatenate((anchor_values, own_values), axis=0)
        allowed = visible(block_number, TOK_DEV, TOK_DEV)
        return block_attention(rows_q, keys_all, values_all, allowed)

    numbers = jnp.arange(blocks, dtype=jnp.int32)
    context = lax.map(phase_one, (numbers, query_blocks, key_blocks, value_blocks))
    context_out = context.reshape(TOKENS, queries.shape[1])

    def phase_two(pieces):
        return block_summary(question, pieces[0], pieces[1])

    highs, totals, mixture = lax.map(phase_two, (key_blocks, value_blocks))
    highest = jnp.max(highs, axis=0)
    factor = jnp.exp(highs - highest)
    denominator = jnp.sum(totals * factor, axis=0)
    numerator = jnp.sum(mixture * factor[..., None], axis=0)
    answer = (numerator / denominator[..., None]).astype(jnp.bfloat16).reshape(QROWS, question.shape[1])
    return context_out, answer
```

```python
import functools
import math

import jax
import jax.numpy as jnp
from jax import lax
from jax.experimental import pallas as pl
from jax.experimental.pallas import tpu as pltpu
from jax.sharding import PartitionSpec as P

HEAD = 128
UNIT = HEAD ** (-0.5) * math.log2(math.e)
LOW = -1e30
MESH = pl.DeviceIdType.MESH


def chip_width(mesh):
    n = mesh.shape["seq"]
    if n < 8 or n % 4:
        return 1
    try:
        row = mesh.devices.reshape(-1, n)[0]
        a, b, c = row[0].coords, row[2].coords, row[4].coords
    except (AttributeError, TypeError):
        return 1
    return 2 if a[1] != b[1] and a[2] == b[2] and a[2] != c[2] and a[1] == c[1] else 1


def trees(n, width):
    long = n // 2 // width
    dev = lambda z, y, core: (z * width + y) * 2 + core
    streams = []
    for x in (0, 1):
        kids = [[] for _ in range(n)]
        if width == 1:
            if x == 0:
                for z in range(long):
                    if z + 1 < long:
                        kids[dev(z, 0, 0)].append(dev(z + 1, 0, 0))
                    kids[dev(z, 0, 0)].append(dev(z, 0, 1))
            else:
                if long > 1:
                    kids[0].append(dev(1, 0, 1))
                kids[0].append(1)
                for z in range(1, long):
                    if z + 1 < long:
                        kids[dev(z, 0, 1)].append(dev(z + 1, 0, 1))
                    kids[dev(z, 0, 1)].append(dev(z, 0, 0))
        else:
            near, far = (0, 1) if x == 0 else (1, 0)
            if x == 1:
                kids[0].extend((dev(0, 1, 1), 1))
            for z in range(long):
                head = dev(z, near, x)
                if z + 1 < long:
                    kids[head].append(dev(z + 1, near, x))
                if z >= 1:
                    kids[head].append(dev(z, far, x))
                kids[head].append(dev(z, near, 1 - x))
                if z >= 1:
                    kids[dev(z, far, x)].append(dev(z, far, 1 - x))
            if x == 0:
                kids[dev(1, 1, 0)].append(dev(0, 1, 0))
                kids[dev(0, 1, 0)].append(dev(0, 1, 1))
        depth = [0.0] * n
        order = [0]
        for d in order:
            for k in kids[d]:
                depth[k] = depth[d] + (0.5 if k // 2 == d // 2 else 1.0)
                order.append(k)
        assert sorted(order) == list(range(n))
        streams.append((kids, depth))
    return streams


def pick(me, table):
    out = jnp.int32(table[0])
    for i in range(1, len(table)):
        if table[i] != table[0]:
            out = jnp.where(me == i, jnp.int32(table[i]), out)
    return out


def kernel(
    n, plan, groups, ratio,
    q_hbm, kv_hbm, qu_hbm, out_hbm, ans_ref,
    q, own, anc, acc, high, den, outv, qu, stack, qn, qb, st, rb, rst, ans,
    q_sem, own_sem, qu_sem, out_sem, a_send, a_recv, n_send, n_recv, s_send, s_recv,
):
    rows = q.shape[0]
    gw = ratio * HEAD
    me = lax.axis_index("seq")
    kid_max = max(len(k) for kids, _ in plan for k in kids)

    barrier = pltpu.get_barrier_semaphore()

    def greet(k, c):
        pl.semaphore_signal(
            barrier, inc=1, device_id={"seq": lax.rem(me + k, n)}, device_id_type=MESH
        )
        return c

    lax.fori_loop(1, n, greet, 0)

    def own_copy(kind, g):
        return pltpu.make_async_copy(
            kv_hbm.at[kind, :, pl.ds(pl.multiple_of(g * HEAD, HEAD), HEAD)],
            own.at[kind * groups + g],
            own_sem.at[kind * groups + g],
        )

    def q_copy(g):
        cols = pl.ds(pl.multiple_of(g * gw, gw), gw)
        return pltpu.make_async_copy(q_hbm.at[:, cols], q.at[:, cols], q_sem.at[g])

    def out_copy(g):
        cols = pl.ds(pl.multiple_of(g * gw, gw), gw)
        return pltpu.make_async_copy(outv.at[:, cols], out_hbm.at[:, cols], out_sem.at[g])

    qu_copy = pltpu.make_async_copy(qu_hbm, qu, qu_sem)
    for g in range(groups):
        own_copy(0, g).start()
        own_copy(1, g).start()
        q_copy(g).start()
    qu_copy.start()

    kids_of = []
    depth_of = []
    for kids, depth in plan:
        padded = [k + [-1] * (kid_max - len(k)) for k in kids]
        kids_of.append([pick(me, [p[j] for p in padded]) for j in range(kid_max)])
        depth_of.append(pick(me, [2 + int(4 * max(d - 1, 0)) for d in depth]))

    pl.semaphore_wait(barrier, n - 1)

    per = groups

    def piece(x, k):
        g = (k // 2) * 2 + x
        kind = lax.rem(k, 2)
        return kind, g, kind * groups + g

    @pl.when(me == 0)
    def _():
        def inject(k, c):
            for x in (0, 1):
                kind, g, idx = piece(x, k)
                for j, kid in enumerate(plan[x][0][0]):
                    pltpu.make_async_remote_copy(
                        src_ref=kv_hbm.at[kind, :, pl.ds(pl.multiple_of(g * HEAD, HEAD), HEAD)],
                        dst_ref=anc.at[idx],
                        send_sem=a_send.at[idx, j],
                        recv_sem=a_recv.at[idx],
                        device_id={"seq": kid},
                        device_id_type=MESH,
                    ).start()
            return c

        lax.fori_loop(0, per, inject, 0)

    def hop(idx, j, kid):
        return pltpu.make_async_remote_copy(
            src_ref=anc.at[idx],
            dst_ref=anc.at[idx],
            send_sem=a_send.at[idx, j],
            recv_sem=a_recv.at[idx],
            device_id={"seq": kid},
            device_id_type=MESH,
        )

    def serve(x, k):
        _, _, idx = piece(x, k)
        hop(idx, 0, jnp.int32(0)).wait_recv()
        for j in range(kid_max):
            kid = kids_of[x][j]

            @pl.when(kid >= 0)
            def _():
                hop(idx, j, kid).start()

    def due(x, slot):
        return jnp.clip((slot - depth_of[x]) // 2, 0, per)

    def serve_range(x, lo, hi):
        @pl.when(me > 0)
        def _():
            lax.fori_loop(lo, hi, lambda k, c: (serve(x, k), c)[1], 0)

    cdims = (((1,), (1,)), ((), ()))
    ones = jnp.ones((rows, HEAD), jnp.bfloat16)
    rb_rows = min(rows, 256)
    pairs = ratio // 2 if ratio % 2 == 0 else ratio
    heads_per = ratio // pairs
    steps = groups * pairs

    def local_step(i, c):
        g = i // pairs
        for x in (0, 1):
            serve_range(x, due(x, i - 1), due(x, i))

        @pl.when(lax.rem(i, pairs) == 0)
        def _():
            own_copy(0, g).wait()
            own_copy(1, g).wait()
            q_copy(g).wait()

        for h in range(heads_per):
            cols = pl.ds(pl.multiple_of((i * heads_per + h) * HEAD, HEAD), HEAD)
            for r0 in range(0, rows, rb_rows):
                rs = pl.ds(r0, rb_rows)
                qt = q[rs, cols]
                key = own[g, pl.ds(0, r0 + rb_rows), :]
                val = own[groups + g, pl.ds(0, r0 + rb_rows), :]
                s = lax.dot_general(qt, key, cdims, preferred_element_type=jnp.float32)
                row_pos = lax.broadcasted_iota(jnp.int32, (rb_rows, rb_rows), 0)
                col_pos = lax.broadcasted_iota(jnp.int32, (rb_rows, rb_rows), 1)
                last = jnp.where(col_pos <= row_pos, s[:, r0:], LOW)
                s = jnp.concatenate((s[:, :r0], last), axis=1) if r0 else last
                m = jnp.max(s, axis=1, keepdims=True)
                p = jnp.exp2((s - m) * UNIT).astype(jnp.bfloat16)
                wide = jnp.concatenate((val, ones[: r0 + rb_rows]), axis=1)
                o = lax.dot(p, wide, preferred_element_type=jnp.float32)
                acc[rs, cols] = o[:, :HEAD]
                den[rs, cols] = o[:, HEAD:]
                high[rs, cols] = jnp.broadcast_to(m, (rb_rows, HEAD))
        return c

    lax.fori_loop(0, steps, local_step, 0)

    qu_copy.wait()
    qrows = qu.shape[0]
    share = qrows // n
    rr = share * ratio

    def question_step(g, c):
        mm, dd = c
        for h in range(ratio):
            cols = pl.ds(pl.multiple_of((g * ratio + h) * HEAD, HEAD), HEAD)
            stack[pl.ds(h, qrows, stride=ratio), :] = qu[:, cols].astype(jnp.float32)
        qt = stack[...].astype(jnp.bfloat16)
        s = lax.dot_general(qt, own[g], cdims, preferred_element_type=jnp.float32)
        m = jnp.max(s, axis=1, keepdims=True)
        p = jnp.exp2((s - m) * UNIT).astype(jnp.bfloat16)
        wide = jnp.concatenate((own[groups + g], ones), axis=1)
        o = lax.dot(p, wide, preferred_element_type=jnp.float32)
        qn[:, g] = o[:, :HEAD].reshape(n, rr, HEAD)
        lane = lax.broadcasted_iota(jnp.int32, (qrows * ratio, HEAD), 1)
        mm = jnp.where(lane == g, m, mm)
        dd = jnp.where(lane == g, o[:, HEAD:], dd)
        return mm, dd

    zero = jnp.zeros((qrows * ratio, HEAD), jnp.float32)
    mm, dd = lax.fori_loop(0, groups, question_step, (zero, zero))
    st[:, 0] = mm.reshape(n, rr, HEAD)
    st[:, 1] = dd.reshape(n, rr, HEAD)

    def narrow(i, c):
        qb[i] = qn[i].reshape(groups * rr, HEAD).astype(jnp.bfloat16)
        return c

    lax.fori_loop(0, n, narrow, 0)

    def exchange(k):
        to = lax.rem(me + k, n)
        return (
            pltpu.make_async_remote_copy(
                src_ref=qb.at[to], dst_ref=rb.at[me], send_sem=n_send.at[to],
                recv_sem=n_recv.at[me], device_id={"seq": to}, device_id_type=MESH,
            ),
            pltpu.make_async_remote_copy(
                src_ref=st.at[to], dst_ref=rst.at[me], send_sem=s_send.at[to],
                recv_sem=s_recv.at[me], device_id={"seq": to}, device_id_type=MESH,
            ),
        )

    def arrived(k):
        frm = lax.rem(me + n - k, n)
        to = lax.rem(me + k, n)
        return (
            pltpu.make_async_remote_copy(
                src_ref=qb.at[to], dst_ref=rb.at[frm], send_sem=n_send.at[to],
                recv_sem=n_recv.at[frm], device_id={"seq": to}, device_id_type=MESH,
            ),
            pltpu.make_async_remote_copy(
                src_ref=st.at[to], dst_ref=rst.at[frm], send_sem=s_send.at[to],
                recv_sem=s_recv.at[frm], device_id={"seq": to}, device_id_type=MESH,
            ),
        )

    def anchor_step(i, c):
        slot = i + steps
        g = i // pairs

        def upto(x, j):
            jg = j // pairs
            asked = jnp.where(j < 0, 0, ((jg + 2 - x) // 2) * 2)
            return jnp.maximum(due(x, j + steps), asked)

        for x in (0, 1):
            serve_range(x, upto(x, i - 1), upto(x, i))

        @pl.when(i == 1)
        def _():
            def go(k, c):
                for copy in exchange(k):
                    copy.start()
                return c

            lax.fori_loop(1, n, go, 0)

        @pl.when(me == 0)
        def _():
            for h in range(heads_per):
                cols = pl.ds(pl.multiple_of((i * heads_per + h) * HEAD, HEAD), HEAD)
                outv[:, cols] = (acc[:, cols] / den[:, cols]).astype(jnp.bfloat16)

        @pl.when(me > 0)
        def _():
            for h in range(heads_per):
                cols = pl.ds(pl.multiple_of((i * heads_per + h) * HEAD, HEAD), HEAD)
                for r0 in range(0, rows, rb_rows):
                    rs = pl.ds(r0, rb_rows)
                    s = lax.dot_general(
                        q[rs, cols], anc[g], cdims, preferred_element_type=jnp.float32
                    )
                    ml = high[rs, cols]
                    m = jnp.maximum(jnp.max(s, axis=1, keepdims=True), ml)
                    mw = jnp.concatenate([m] * (s.shape[1] // HEAD), axis=1)
                    p = jnp.exp2((s - mw) * UNIT).astype(jnp.bfloat16)
                    wide = jnp.concatenate((anc[groups + g], ones), axis=1)
                    o = lax.dot(p, wide, preferred_element_type=jnp.float32)
                    f = jnp.exp2((ml - m) * UNIT)
                    num = o[:, :HEAD] + f * acc[rs, cols]
                    total = o[:, HEAD:] + f * den[rs, cols]
                    outv[rs, cols] = (num / total).astype(jnp.bfloat16)

        @pl.when(lax.rem(i, pairs) == pairs - 1)
        def _():
            out_copy(g).start()

        return c

    lax.fori_loop(0, steps, anchor_step, 0)

    rb[me] = qb[me]
    rst[me] = st[me]

    def land(k, c):
        for copy in arrived(k):
            copy.wait()
        return c

    lax.fori_loop(1, n, land, 0)

    top = lax.fori_loop(1, n, lambda j, t: jnp.maximum(t, rst[j, 0]), rst[0, 0])

    def gather(j, c):
        total, nums = c
        w = jnp.exp2((rst[j, 0] - top) * UNIT)
        total = total + w * rst[j, 1]
        part = rb[j].astype(jnp.float32)
        nums = tuple(
            nums[g] + w[:, g : g + 1] * part[g * rr : (g + 1) * rr] for g in range(groups)
        )
        return total, nums

    tile = jnp.zeros((rr, HEAD), jnp.float32)
    total, nums = lax.fori_loop(0, n, gather, (tile, (tile,) * groups))
    for g in range(groups):
        mine = nums[g] / total[:, g : g + 1]
        for r in range(share):
            for h in range(ratio):
                k = r * ratio + h
                ans[r : r + 1, (g * ratio + h) * HEAD : (g * ratio + h + 1) * HEAD] = mine[k : k + 1]
    ans_ref[...] = ans[...].astype(jnp.bfloat16)

    def sent(idx, c):
        g = lax.rem(idx, groups)
        for x in (0, 1):
            for j in range(kid_max):

                @pl.when((lax.rem(g, 2) == x) & (kids_of[x][j] >= 0))
                def _():
                    hop(idx, j, jnp.maximum(kids_of[x][j], 0)).wait_send()

        return c

    lax.fori_loop(0, 2 * groups, sent, 0)
    for g in range(groups):
        out_copy(g).wait()


def solution(mesh):
    n = mesh.shape["seq"]
    plan = trees(n, chip_width(mesh))
    kid_max = max(len(k) for kids, _ in plan for k in kids)

    def on_device(queries, kv_cache, question):
        rows, width = queries.shape
        groups = kv_cache.shape[2] // HEAD
        ratio = width // kv_cache.shape[2]
        qrows = question.shape[0]
        share = qrows // n
        rr = share * ratio
        any_space = pl.BlockSpec(memory_space=pl.ANY)
        dma = pltpu.SemaphoreType.DMA
        return pl.pallas_call(
            functools.partial(kernel, n, plan, groups, ratio),
            out_shape=(
                jax.ShapeDtypeStruct((rows, width), jnp.bfloat16),
                jax.ShapeDtypeStruct((share, width), jnp.bfloat16),
            ),
            in_specs=[any_space] * 3,
            out_specs=(any_space, pl.BlockSpec(memory_space=pltpu.VMEM)),
            scratch_shapes=[
                pltpu.VMEM((rows, width), jnp.bfloat16),
                pltpu.VMEM((2 * groups, rows, HEAD), jnp.bfloat16),
                pltpu.VMEM((2 * groups, rows, HEAD), jnp.bfloat16),
                pltpu.VMEM((rows, width), jnp.float32),
                pltpu.VMEM((rows, width), jnp.float32),
                pltpu.VMEM((rows, width), jnp.float32),
                pltpu.VMEM((rows, width), jnp.bfloat16),
                pltpu.VMEM((qrows, width), jnp.bfloat16),
                pltpu.VMEM((qrows * ratio, HEAD), jnp.float32),
                pltpu.VMEM((n, groups, rr, HEAD), jnp.float32),
                pltpu.VMEM((n, groups * rr, HEAD), jnp.bfloat16),
                pltpu.VMEM((n, 2, rr, HEAD), jnp.float32),
                pltpu.VMEM((n, groups * rr, HEAD), jnp.bfloat16),
                pltpu.VMEM((n, 2, rr, HEAD), jnp.float32),
                pltpu.VMEM((share, width), jnp.float32),
                dma((groups,)),
                dma((2 * groups,)),
                dma,
                dma((groups,)),
                dma((2 * groups, kid_max)),
                dma((2 * groups,)),
                dma((n,)),
                dma((n,)),
                dma((n,)),
                dma((n,)),
            ],
            compiler_params=pltpu.CompilerParams(
                collective_id=0, has_side_effects=True, vmem_limit_bytes=56 * 2**20
            ),
        )(queries, kv_cache, question)

    return jax.shard_map(
        on_device,
        mesh=mesh,
        in_specs=(P(("grp", "seq"), None), P(None, ("grp", "seq"), None), P("grp", None)),
        out_specs=(P(("grp", "seq"), None), P(("grp", "seq"), None)),
        check_vma=False,
    )
```

```python
import functools
import math

import jax
import jax.numpy as jnp
from jax import lax
from jax.experimental import pallas as pl
from jax.experimental.pallas import tpu as pltpu
from jax.sharding import PartitionSpec as P

HEAD = 128
UNIT = HEAD ** (-0.5) * math.log2(math.e)
LOW = -1e30
MESH = pl.DeviceIdType.MESH


def chip_width(mesh):
    n = mesh.shape["seq"]
    if n < 8 or n % 4:
        return 1
    try:
        row = mesh.devices.reshape(-1, n)[0]
        a, b, c = row[0].coords, row[2].coords, row[4].coords
    except (AttributeError, TypeError):
        return 1
    return 2 if a[1] != b[1] and a[2] == b[2] and a[2] != c[2] and a[1] == c[1] else 1


def trees(n, width):
    long = n // 2 // width
    dev = lambda z, y, core: (z * width + y) * 2 + core
    streams = []
    for x in (0, 1):
        kids = [[] for _ in range(n)]
        if width == 1:
            if x == 0:
                for z in range(long):
                    if z + 1 < long:
                        kids[dev(z, 0, 0)].append(dev(z + 1, 0, 0))
                    kids[dev(z, 0, 0)].append(dev(z, 0, 1))
            else:
                if long > 1:
                    kids[0].append(dev(1, 0, 1))
                kids[0].append(1)
                for z in range(1, long):
                    if z + 1 < long:
                        kids[dev(z, 0, 1)].append(dev(z + 1, 0, 1))
                    kids[dev(z, 0, 1)].append(dev(z, 0, 0))
        else:
            near, far = (0, 1) if x == 0 else (1, 0)
            if x == 1:
                kids[0].extend((dev(0, 1, 1), 1))
            for z in range(long):
                head = dev(z, near, x)
                if z + 1 < long:
                    kids[head].append(dev(z + 1, near, x))
                if z >= 1:
                    kids[head].append(dev(z, far, x))
                kids[head].append(dev(z, near, 1 - x))
                if z >= 1:
                    kids[dev(z, far, x)].append(dev(z, far, 1 - x))
            if x == 0:
                kids[dev(1, 1, 0)].append(dev(0, 1, 0))
                kids[dev(0, 1, 0)].append(dev(0, 1, 1))
        depth = [0.0] * n
        order = [0]
        for d in order:
            for k in kids[d]:
                depth[k] = depth[d] + (0.5 if k // 2 == d // 2 else 1.0)
                order.append(k)
        assert sorted(order) == list(range(n))
        streams.append((kids, depth))
    return streams


def pick(me, table):
    out = jnp.int32(table[0])
    for i in range(1, len(table)):
        if table[i] != table[0]:
            out = jnp.where(me == i, jnp.int32(table[i]), out)
    return out


def kernel(
    n, plan, groups, ratio,
    q_hbm, kv_hbm, qu_hbm, out_hbm, ans_ref,
    q, own, anc, acc, high, den, outv, qu, stack, qn, qb, st, rb, rst, ans,
    q_sem, own_sem, qu_sem, out_sem, a_send, a_recv, n_send, n_recv, s_send, s_recv,
):
    rows = q.shape[0]
    gw = ratio * HEAD
    me = lax.axis_index("seq")
    kid_max = max(len(k) for kids, _ in plan for k in kids)

    barrier = pltpu.get_barrier_semaphore()

    def greet(k, c):
        pl.semaphore_signal(
            barrier, inc=1, device_id={"seq": lax.rem(me + k, n)}, device_id_type=MESH
        )
        return c

    lax.fori_loop(1, n, greet, 0)

    def own_copy(kind, g):
        return pltpu.make_async_copy(
            kv_hbm.at[kind, :, pl.ds(pl.multiple_of(g * HEAD, HEAD), HEAD)],
            own.at[kind * groups + g],
            own_sem.at[kind * groups + g],
        )

    def q_copy(g):
        cols = pl.ds(pl.multiple_of(g * gw, gw), gw)
        return pltpu.make_async_copy(q_hbm.at[:, cols], q.at[:, cols], q_sem.at[g])

    def out_copy(g):
        cols = pl.ds(pl.multiple_of(g * gw, gw), gw)
        return pltpu.make_async_copy(outv.at[:, cols], out_hbm.at[:, cols], out_sem.at[g])

    qu_copy = pltpu.make_async_copy(qu_hbm, qu, qu_sem)
    qu_copy.start()
    for g in range(groups):
        own_copy(0, g).start()
        own_copy(1, g).start()
    for g in range(groups):
        q_copy(g).start()

    kids_of = []
    depth_of = []
    for kids, depth in plan:
        padded = [k + [-1] * (kid_max - len(k)) for k in kids]
        kids_of.append([pick(me, [p[j] for p in padded]) for j in range(kid_max)])
        depth_of.append(pick(me, [int(2 * max(d - 1, 0)) for d in depth]))

    pl.semaphore_wait(barrier, n - 1)

    per = groups

    def piece(x, k):
        g = (k // 2) * 2 + x
        kind = lax.rem(k, 2)
        return kind, g, kind * groups + g

    @pl.when(me == 0)
    def _():
        def inject(k, c):
            for x in (0, 1):
                kind, g, idx = piece(x, k)
                for j, kid in enumerate(plan[x][0][0]):
                    pltpu.make_async_remote_copy(
                        src_ref=kv_hbm.at[kind, :, pl.ds(pl.multiple_of(g * HEAD, HEAD), HEAD)],
                        dst_ref=anc.at[idx],
                        send_sem=a_send.at[idx, j],
                        recv_sem=a_recv.at[idx],
                        device_id={"seq": kid},
                        device_id_type=MESH,
                    ).start()
            return c

        lax.fori_loop(0, per, inject, 0)

    def hop(idx, j, kid):
        return pltpu.make_async_remote_copy(
            src_ref=anc.at[idx],
            dst_ref=anc.at[idx],
            send_sem=a_send.at[idx, j],
            recv_sem=a_recv.at[idx],
            device_id={"seq": kid},
            device_id_type=MESH,
        )

    def serve(x, k):
        _, _, idx = piece(x, k)
        hop(idx, 0, jnp.int32(0)).wait_recv()
        for j in range(kid_max):
            kid = kids_of[x][j]

            @pl.when(kid >= 0)
            def _():
                hop(idx, j, kid).start()

    def due(x, slot):
        late = slot - depth_of[x]
        return jnp.where(late < 0, 0, jnp.minimum((late * 6 + 9) // 5, per))

    def serve_range(x, lo, hi):
        @pl.when(me > 0)
        def _():
            lax.fori_loop(lo, hi, lambda k, c: (serve(x, k), c)[1], 0)

    cdims = (((1,), (1,)), ((), ()))
    ones = jnp.ones((rows, HEAD), jnp.bfloat16)
    rb_rows = min(rows, 256)
    pairs = 1
    heads_per = ratio
    steps = groups

    qu_copy.wait()
    for g in range(groups):
        own_copy(0, g).wait()
        own_copy(1, g).wait()
    qrows = qu.shape[0]
    share = qrows // n
    rr = share * ratio

    def question_step(g, c):
        mm, dd = c
        for h in range(ratio):
            cols = pl.ds(pl.multiple_of((g * ratio + h) * HEAD, HEAD), HEAD)
            stack[lax.rem(g, 4), pl.ds(h, qrows, stride=ratio), :] = qu[:, cols].astype(jnp.float32)
        qt = stack[lax.rem(g, 4)].astype(jnp.bfloat16)
        s = lax.dot_general(qt, own[g], cdims, preferred_element_type=jnp.float32)
        m = jnp.max(s, axis=1, keepdims=True)
        p = jnp.exp2((s - m) * UNIT).astype(jnp.bfloat16)
        wide = jnp.concatenate((own[groups + g], ones), axis=1)
        o = lax.dot(p, wide, preferred_element_type=jnp.float32)
        qn[:, g] = o[:, :HEAD].reshape(n, rr, HEAD)
        lane = lax.broadcasted_iota(jnp.int32, (qrows * ratio, HEAD), 1)
        mm = jnp.where(lane == g, m, mm)
        dd = jnp.where(lane == g, o[:, HEAD:], dd)
        return mm, dd

    zero = jnp.zeros((qrows * ratio, HEAD), jnp.float32)
    mm, dd = lax.fori_loop(0, groups, question_step, (zero, zero), unroll=4)
    st[:, 0] = mm.reshape(n, rr, HEAD)
    st[:, 1] = dd.reshape(n, rr, HEAD)

    def narrow(i, c):
        qb[i] = qn[i].reshape(groups * rr, HEAD).astype(jnp.bfloat16)
        return c

    lax.fori_loop(0, n, narrow, 0, unroll=4)

    def local_step(i, c):
        g = i // pairs
        for x in (0, 1):
            serve_range(x, due(x, i - 1), due(x, i))

        @pl.when(lax.rem(i, pairs) == 0)
        def _():
            q_copy(g).wait()

        for h in range(heads_per):
            cols = pl.ds(pl.multiple_of((i * heads_per + h) * HEAD, HEAD), HEAD)
            for r0 in range(0, rows, rb_rows):
                rs = pl.ds(r0, rb_rows)
                qt = q[rs, cols]
                key = own[g, pl.ds(0, r0 + rb_rows), :]
                val = own[groups + g, pl.ds(0, r0 + rb_rows), :]
                s = lax.dot_general(qt, key, cdims, preferred_element_type=jnp.float32)
                row_pos = lax.broadcasted_iota(jnp.int32, (rb_rows, rb_rows), 0)
                col_pos = lax.broadcasted_iota(jnp.int32, (rb_rows, rb_rows), 1)
                last = jnp.where(col_pos <= row_pos, s[:, r0:], LOW)
                s = jnp.concatenate((s[:, :r0], last), axis=1) if r0 else last
                m = jnp.max(s, axis=1, keepdims=True)
                p = jnp.exp2((s - m) * UNIT).astype(jnp.bfloat16)
                wide = jnp.concatenate((val, ones[: r0 + rb_rows]), axis=1)
                o = lax.dot(p, wide, preferred_element_type=jnp.float32)
                acc[rs, cols] = o[:, :HEAD]
                den[rs, cols] = o[:, HEAD:]
                high[rs, cols] = jnp.broadcast_to(m, (rb_rows, HEAD))
        return c

    lax.fori_loop(0, steps, local_step, 0)

    def exchange(k):
        to = lax.rem(me + k, n)
        return (
            pltpu.make_async_remote_copy(
                src_ref=qb.at[to], dst_ref=rb.at[me], send_sem=n_send.at[to],
                recv_sem=n_recv.at[me], device_id={"seq": to}, device_id_type=MESH,
            ),
            pltpu.make_async_remote_copy(
                src_ref=st.at[to], dst_ref=rst.at[me], send_sem=s_send.at[to],
                recv_sem=s_recv.at[me], device_id={"seq": to}, device_id_type=MESH,
            ),
        )

    def arrived(k):
        frm = lax.rem(me + n - k, n)
        to = lax.rem(me + k, n)
        return (
            pltpu.make_async_remote_copy(
                src_ref=qb.at[to], dst_ref=rb.at[frm], send_sem=n_send.at[to],
                recv_sem=n_recv.at[frm], device_id={"seq": to}, device_id_type=MESH,
            ),
            pltpu.make_async_remote_copy(
                src_ref=st.at[to], dst_ref=rst.at[frm], send_sem=s_send.at[to],
                recv_sem=s_recv.at[frm], device_id={"seq": to}, device_id_type=MESH,
            ),
        )

    def anchor_step(i, c):
        slot = i + steps
        g = i // pairs

        def upto(x, j):
            jg = j // pairs
            asked = jnp.where(j < 0, 0, ((jg + 2 - x) // 2) * 2)
            return jnp.maximum(due(x, j + steps), asked)

        for x in (0, 1):
            serve_range(x, upto(x, i - 1), upto(x, i))

        @pl.when(i == 2)
        def _():
            def go(k, c):
                for copy in exchange(k):
                    copy.start()
                return c

            lax.fori_loop(1, n, go, 0)

        @pl.when(me == 0)
        def _():
            for h in range(heads_per):
                cols = pl.ds(pl.multiple_of((i * heads_per + h) * HEAD, HEAD), HEAD)
                outv[:, cols] = (acc[:, cols] / den[:, cols]).astype(jnp.bfloat16)

        @pl.when(me > 0)
        def _():
            for h in range(heads_per):
                cols = pl.ds(pl.multiple_of((i * heads_per + h) * HEAD, HEAD), HEAD)
                for r0 in range(0, rows, rb_rows):
                    rs = pl.ds(r0, rb_rows)
                    s = lax.dot_general(
                        q[rs, cols], anc[g], cdims, preferred_element_type=jnp.float32
                    )
                    ml = high[rs, cols]
                    m = jnp.maximum(jnp.max(s, axis=1, keepdims=True), ml)
                    mw = jnp.concatenate([m] * (s.shape[1] // HEAD), axis=1)
                    p = jnp.exp2((s - mw) * UNIT).astype(jnp.bfloat16)
                    wide = jnp.concatenate((anc[groups + g], ones), axis=1)
                    o = lax.dot(p, wide, preferred_element_type=jnp.float32)
                    f = jnp.exp2((ml - m) * UNIT)
                    num = o[:, :HEAD] + f * acc[rs, cols]
                    total = o[:, HEAD:] + f * den[rs, cols]
                    outv[rs, cols] = (num / total).astype(jnp.bfloat16)

        @pl.when(lax.rem(i, pairs) == pairs - 1)
        def _():
            out_copy(g).start()

        return c

    lax.fori_loop(0, steps, anchor_step, 0)

    rb[me] = qb[me]
    rst[me] = st[me]

    def land(k, c):
        for copy in arrived(k):
            copy.wait()
        return c

    lax.fori_loop(1, n, land, 0)

    top = lax.fori_loop(1, n, lambda j, t: jnp.maximum(t, rst[j, 0]), rst[0, 0])

    def gather(j, c):
        total, nums = c
        w = jnp.exp2((rst[j, 0] - top) * UNIT)
        total = total + w * rst[j, 1]
        part = rb[j].astype(jnp.float32)
        nums = tuple(
            nums[g] + w[:, g : g + 1] * part[g * rr : (g + 1) * rr] for g in range(groups)
        )
        return total, nums

    tile = jnp.zeros((rr, HEAD), jnp.float32)
    total, nums = lax.fori_loop(0, n, gather, (tile, (tile,) * groups), unroll=2)
    for g in range(groups):
        mine = nums[g] / total[:, g : g + 1]
        for r in range(share):
            for h in range(ratio):
                k = r * ratio + h
                ans[r : r + 1, (g * ratio + h) * HEAD : (g * ratio + h + 1) * HEAD] = mine[k : k + 1]
    ans_ref[...] = ans[...].astype(jnp.bfloat16)

    def sent(idx, c):
        g = lax.rem(idx, groups)
        for x in (0, 1):
            for j in range(kid_max):

                @pl.when((lax.rem(g, 2) == x) & (kids_of[x][j] >= 0))
                def _():
                    hop(idx, j, jnp.maximum(kids_of[x][j], 0)).wait_send()

        return c

    lax.fori_loop(0, 2 * groups, sent, 0)
    for g in range(groups):
        out_copy(g).wait()


def solution(mesh):
    n = mesh.shape["seq"]
    plan = trees(n, chip_width(mesh))
    kid_max = max(len(k) for kids, _ in plan for k in kids)

    def on_device(queries, kv_cache, question):
        rows, width = queries.shape
        groups = kv_cache.shape[2] // HEAD
        ratio = width // kv_cache.shape[2]
        qrows = question.shape[0]
        share = qrows // n
        rr = share * ratio
        any_space = pl.BlockSpec(memory_space=pl.ANY)
        dma = pltpu.SemaphoreType.DMA
        return pl.pallas_call(
            functools.partial(kernel, n, plan, groups, ratio),
            out_shape=(
                jax.ShapeDtypeStruct((rows, width), jnp.bfloat16),
                jax.ShapeDtypeStruct((share, width), jnp.bfloat16),
            ),
            in_specs=[any_space] * 3,
            out_specs=(any_space, pl.BlockSpec(memory_space=pltpu.VMEM)),
            scratch_shapes=[
                pltpu.VMEM((rows, width), jnp.bfloat16),
                pltpu.VMEM((2 * groups, rows, HEAD), jnp.bfloat16),
                pltpu.VMEM((2 * groups, rows, HEAD), jnp.bfloat16),
                pltpu.VMEM((rows, width), jnp.float32),
                pltpu.VMEM((rows, width), jnp.float32),
                pltpu.VMEM((rows, width), jnp.float32),
                pltpu.VMEM((rows, width), jnp.bfloat16),
                pltpu.VMEM((qrows, width), jnp.bfloat16),
                pltpu.VMEM((4, qrows * ratio, HEAD), jnp.float32),
                pltpu.VMEM((n, groups, rr, HEAD), jnp.float32),
                pltpu.VMEM((n, groups * rr, HEAD), jnp.bfloat16),
                pltpu.VMEM((n, 2, rr, HEAD), jnp.float32),
                pltpu.VMEM((n, groups * rr, HEAD), jnp.bfloat16),
                pltpu.VMEM((n, 2, rr, HEAD), jnp.float32),
                pltpu.VMEM((share, width), jnp.float32),
                dma((groups,)),
                dma((2 * groups,)),
                dma,
                dma((groups,)),
                dma((2 * groups, kid_max)),
                dma((2 * groups,)),
                dma((n,)),
                dma((n,)),
                dma((n,)),
                dma((n,)),
            ],
            compiler_params=pltpu.CompilerParams(
                collective_id=0, has_side_effects=True, vmem_limit_bytes=56 * 2**20
            ),
        )(queries, kv_cache, question)

    return jax.shard_map(
        on_device,
        mesh=mesh,
        in_specs=(P(("grp", "seq"), None), P(None, ("grp", "seq"), None), P("grp", None)),
        out_specs=(P(("grp", "seq"), None), P(("grp", "seq"), None)),
        check_vma=False,
    )
```
